256 devices in a mesh: seq: 16 (over z, core), dp: 16 (over x, y).
Axes of the slice: x: 4, y: 4, z: 8, core: 2. Of those that a mesh axis runs over, the one named last changes fastest.
Arguments:
- raw_query: bfloat16 [16, 4096, 2048], P('dp', 'seq'), may hold values from -4 to 4
- raw_key: bfloat16 [16, 4096, 2048], P('dp', 'seq'), may hold values from -4 to 4
- raw_value: bfloat16 [16, 4096, 2048], P('dp', 'seq'), may hold values from -6 to 6
- query_gain: float32 [128], replicated, may hold values from 0.5 to 8
- key_gain: float32 [128], replicated, may hold values from 0.5 to 8
- lengths: int32 [64], replicated, may hold values from 1 to 4096, 65536 in all
- clip_grids: int32 [64, 2], replicated, may hold values from 4 to 23
Outputs:
- attended: bfloat16 [16, 4096, 2048], P('dp', 'seq')
The draws below stay inside these ranges and needn't reach their ends.
All inputs are finite; a program needn't handle non-finite values.
Results may differ from the reference program's by a relative error of at most 0.0017.
The reference program's roundings to bfloat16 on the way count: a program that leaves them out, or rounds other values in their place, can miss the bound.
Values may be sent and summed in bfloat16 or wider, within the bound.
No kernel may reach another device: no remote copies, remote signals or barrier semaphores. Data moves between devices by JAX's collectives and lax.ppermute only.
A program may use at most 64 MiB of HBM per device.

```python
import math
import jax
import jax.numpy as jnp
import numpy as np
from jax import lax

HEADS = 16
HEAD_DIM = 128
PACK = 4096
PACKS = 16
TOKENS = 65536
WIDTH = 2048
MOST = 4096
CLIPS = 64


def query_key_pair(key):
    base_key = jax.random.fold_in(key, 17)
    first_key, second_key = jax.random.split(base_key, 2)
    shape = (PACKS, PACK, WIDTH)
    key_part = jax.random.truncated_normal(first_key, -4.0, 4.0, shape, jnp.float32)
    query_part = jax.random.truncated_normal(second_key, -4.0, 4.0, shape, jnp.float32)
    return (query_part, key_part)


def draw_raw_query(key, part):
    return query_key_pair(key)[0].astype(jnp.bfloat16)


def draw_raw_key(key, part):
    return query_key_pair(key)[1].astype(jnp.bfloat16)


def gain_draw(key, salt):
    sub_key = jax.random.fold_in(key, salt)
    low_end, high_end = (0.5, 2.0)
    return jnp.exp(jax.random.uniform(sub_key, (HEAD_DIM,), jnp.float32, math.log(low_end), math.log(high_end)))


def draw_query_gain(key, part):
    return gain_draw(key, 31)


def draw_key_gain(key, part):
    return gain_draw(key, 43)


def touch_ends(values, rng, low, high):
    shape = values.shape
    spot = [jax.random.randint(jax.random.fold_in(rng, axis), (), 0, shape[axis]) for axis in range(len(shape))]
    values = values.at[tuple(spot)].set(low)
    longest = shape.index(max(shape))
    spot[longest] = (spot[longest] + 1) % shape[longest]
    return values.at[tuple(spot)].set(high)


def steps_of(rng, extent, cuts, low, high):
    def one(position, parts):
        steps = jax.random.uniform(jax.random.fold_in(jax.random.fold_in(rng, 6), position), (parts,), jnp.float32, low / len(cuts), high / len(cuts))
        return jnp.repeat(jnp.exp(steps), extent[position] // parts).reshape((-1,) + (1,) * (len(extent) - position - 1))

    gain = one(*cuts[0])
    for cut in cuts[1:]:
        gain = gain * one(*cut)
    return gain


def length_profile(count, total, most, slope):
    weights = [(1 << 20) // math.isqrt(grade ** slope) + 1 for grade in range(2, count + 1)]
    spare, holding = total - most - (count - 1), [1] * (count - 1)
    while spare > 0:
        free = [i for i in range(count - 1) if holding[i] < most]
        pool, budget = sum([weights[i] for i in free]), spare
        for i in free:
            addition = min(most - holding[i], max(1, budget * weights[i] // pool), spare)
            holding[i] = holding[i] + addition
            spare = spare - addition
    return np.array([most] + holding)


def uneven_parts(key, number_of, total, bound, lean):
    if number_of == 2:
        one = jax.random.randint(key, (), max(1, total - bound), min(bound, total - 1) + 1)
        return jnp.stack([one, total - one])
    sizes = jnp.asarray(length_profile(number_of, total, bound, lean), jnp.int32)
    couples = (number_of - 1) // 2
    giver, sink = sizes[1:1 + 2 * couples:2], sizes[2:2 + 2 * couples:2]
    room = jnp.minimum(giver - 1, bound - sink)
    passed = jax.random.randint(jax.random.fold_in(key, 1), (couples,), 0, 1 << 20) % (room + 1)
    sizes = sizes.at[1:1 + 2 * couples:2].set(giver - passed).at[2:2 + 2 * couples:2].set(sink + passed)
    return sizes[jax.random.permutation(jax.random.fold_in(key, 2), number_of)]


def normal_values(key, dims, spread, reach, cuts=(), kind=jnp.bfloat16):
    gain = steps_of(key, dims, cuts, -0.22, 0.18) if cuts else 1.0
    array = jax.random.normal(key, dims, jnp.float32) * spread * gain
    return jnp.minimum(jnp.maximum(array, -reach), reach).astype(kind)


def setup_inputs(seed: int = 0) -> dict:
    arg_keys = jax.random.split(jax.random.key(seed), 8)
    raw_query = draw_raw_query(jax.random.fold_in(arg_keys[7], 71), 0)
    raw_key = draw_raw_key(jax.random.fold_in(arg_keys[7], 71), 0)
    raw_value = normal_values(arg_keys[2], (PACKS, PACK, WIDTH), 1.0, 6.0, ((0, 16), (1, 16)))
    query_gain = draw_query_gain(jax.random.fold_in(arg_keys[7], 71), 0)
    key_gain = draw_key_gain(jax.random.fold_in(arg_keys[7], 71), 0)
    lengths = uneven_parts(arg_keys[5], CLIPS, TOKENS, MOST, 2).astype(jnp.int32)
    clip_grids = touch_ends(jax.random.randint(arg_keys[6], (CLIPS, 2), 4, 24), jax.random.fold_in(arg_keys[6], 1), 4, 23).astype(jnp.int32)
    return dict(raw_query=raw_query, raw_key=raw_key, raw_value=raw_value, query_gain=query_gain, key_gain=key_gain, lengths=lengths, clip_grids=clip_grids)


NORM_EPS = 1e-06
ROPE_THETA = 256.0
SCORE_SCALE = 1.0 / math.sqrt(128.0)
MASK_FLOOR = -1e+30

def angle_rates():
    pair_num = jnp.arange(128, dtype=jnp.int32) // 2
    pair_real = pair_num.astype(jnp.float32)
    time_rate = jnp.where(pair_num < 8, ROPE_THETA ** (-2.0 * pair_real / 16.0), 0.0)
    height_rate = jnp.where((pair_num >= 8) & (pair_num < 36), ROPE_THETA ** (-2.0 * (pair_real - 8.0) / 56.0), 0.0)
    width_rate = jnp.where(pair_num >= 36, ROPE_THETA ** (-2.0 * (pair_real - 36.0) / 56.0), 0.0)
    return (time_rate, height_rate, width_rate)

def clip_lookup(global_row, lengths):
    clip_ends = jnp.cumsum(lengths).astype(jnp.int32)
    clip_starts = (clip_ends - lengths).astype(jnp.int32)
    clip_id = lax.optimization_barrier(jnp.sum((global_row[:, None] >= clip_ends[None, :]).astype(jnp.int32), axis=1)).astype(jnp.int32)
    one_hot = (clip_id[:, None] == jnp.arange(lengths.shape[0], dtype=jnp.int32)[None, :]).astype(jnp.int32)
    clip_start = lax.optimization_barrier(jnp.sum(one_hot * clip_starts[None, :], axis=1)).astype(jnp.int32)
    clip_end = lax.optimization_barrier(jnp.sum(one_hot * clip_ends[None, :], axis=1)).astype(jnp.int32)
    return (clip_id, clip_start, clip_end, one_hot)

def rope_tables(lookup, global_row, clip_grids):
    clip_start = lookup[1]
    one_hot = lookup[3]
    height = lax.optimization_barrier(jnp.sum(one_hot * clip_grids[None, :, 0], axis=1)).astype(jnp.int32)
    breadth = lax.optimization_barrier(jnp.sum(one_hot * clip_grids[None, :, 1], axis=1)).astype(jnp.int32)
    offset = global_row - clip_start
    frame_pos = offset // (height * breadth)
    row_pos = offset // breadth % height
    col_pos = offset % breadth
    time_rate, height_rate, width_rate = angle_rates()
    angles = frame_pos.astype(jnp.float32)[:, None] * time_rate[None, :] + row_pos.astype(jnp.float32)[:, None] * height_rate[None, :] + col_pos.astype(jnp.float32)[:, None] * width_rate[None, :]
    return (jnp.cos(angles)[:, None, :], jnp.sin(angles)[:, None, :])

def prepare(raw_rows, gain_vec, cosine_part, sine_part):
    as_float = raw_rows.astype(jnp.float32)
    scaled = as_float * lax.rsqrt(lax.optimization_barrier(jnp.mean(as_float * as_float, axis=-1, keepdims=True)) + NORM_EPS) * gain_vec
    pair_view = scaled.reshape(scaled.shape[:-1] + (64, 2))
    swapped = jnp.stack([-pair_view[..., 1], pair_view[..., 0]], axis=-1).reshape(scaled.shape)
    return (scaled * cosine_part + swapped * sine_part).astype(jnp.bfloat16)

def attend(queries, query_clip, key_rows, value_rows, key_clip, low_tile, high_tile, tile_rows):
    row_count = queries.shape[0]
    head_count = queries.shape[1]
    query_wide = queries.astype(jnp.float32)
    start_carry = (jnp.full((row_count, head_count), MASK_FLOOR, jnp.float32), jnp.zeros((row_count, head_count), jnp.float32), jnp.zeros((row_count, head_count, queries.shape[2]), jnp.float32))

    def visit_tile(tile_num, tile_carry):
        row_max, row_sum, weighted = tile_carry
        key_start = tile_num * tile_rows
        key_tile = lax.dynamic_slice_in_dim(key_rows, key_start, tile_rows, 0).astype(jnp.float32)
        value_tile = lax.dynamic_slice_in_dim(value_rows, key_start, tile_rows, 0)
        clip_tile = lax.dynamic_slice_in_dim(key_clip, key_start, tile_rows, 0)
        scores = jnp.einsum('qhd,khd->qhk', query_wide, key_tile) * SCORE_SCALE
        same_clip = (query_clip[:, None] == clip_tile[None, :])[:, None, :]
        new_max = jnp.maximum(row_max, lax.optimization_barrier(jnp.max(jnp.where(same_clip, scores, MASK_FLOOR), axis=2)))
        weights = jnp.where(same_clip, jnp.exp(scores - new_max[..., None]), 0.0)
        shrink = jnp.exp(row_max - new_max)
        row_sum = row_sum * shrink + lax.optimization_barrier(jnp.sum(weights, axis=2))
        rounded = weights.astype(jnp.bfloat16).astype(jnp.float32)
        weighted = weighted * shrink[..., None] + jnp.einsum('qhk,khd->qhd', rounded, value_tile.astype(jnp.float32))
        return (new_max, row_sum, weighted)
    row_max, row_sum, weighted = lax.fori_loop(low_tile, high_tile, visit_tile, start_carry)
    return (row_sum, weighted)

def attend_rows(queries, query_clip, low_tiles, high_tiles, key_rows, value_rows, key_clip, tile_rows):
    tile_count = queries.shape[0] // tile_rows

    def one_tile(tile_num):
        query_tile = lax.dynamic_slice_in_dim(queries, tile_num * tile_rows, tile_rows, 0)
        clip_tile = lax.dynamic_slice_in_dim(query_clip, tile_num * tile_rows, tile_rows, 0)
        low_tile = lax.dynamic_index_in_dim(low_tiles, tile_num, keepdims=False)
        high_tile = lax.dynamic_index_in_dim(high_tiles, tile_num, keepdims=False)
        row_sum, weighted = attend(query_tile, clip_tile, key_rows, value_rows, key_clip, low_tile, high_tile, tile_rows)
        return (weighted / row_sum[..., None]).astype(jnp.bfloat16)
    tiles_out = lax.map(one_tile, jnp.arange(tile_count, dtype=jnp.int32))
    return tiles_out.reshape(queries.shape)

def reference(raw_query, raw_key, raw_value, query_gain, key_gain, lengths, clip_grids):
    global_row = jnp.arange(TOKENS, dtype=jnp.int32)
    lookup = clip_lookup(global_row, lengths)
    cosine_part, sine_part = rope_tables(lookup, global_row, clip_grids)
    queries = prepare(raw_query.reshape(TOKENS, HEADS, HEAD_DIM), query_gain, cosine_part, sine_part)
    key_rows = prepare(raw_key.reshape(TOKENS, HEADS, HEAD_DIM), key_gain, cosine_part, sine_part)
    value_rows = raw_value.reshape(TOKENS, HEADS, HEAD_DIM)
    tile_rows = math.gcd(PACK, 512)
    clip_id, clip_start, clip_end = (lookup[0], lookup[1], lookup[2])
    low_tiles = (clip_start.reshape(-1, tile_rows)[:, 0] // tile_rows).astype(jnp.int32)
    high_tiles = ((clip_end.reshape(-1, tile_rows)[:, -1] + tile_rows - 1) // tile_rows).astype(jnp.int32)
    attended = attend_rows(queries, clip_id, low_tiles, high_tiles, key_rows, value_rows, clip_id, tile_rows)
    return attended.reshape(PACKS, PACK, WIDTH)
```

```python
import functools
import math

import jax
import jax.numpy as jnp
import numpy as np
from jax import lax
from jax.experimental import pallas as pl
from jax.experimental.pallas import tpu as pltpu
from jax.sharding import Mesh
from jax.sharding import PartitionSpec as P


NORM_EPS = 1e-06
ROPE_THETA = 256.0
SCORE_SCALE = 1.0 / math.sqrt(128.0)
MASK_FLOOR = -1e30
EXP2_SCALE = SCORE_SCALE * math.log2(math.e)
TILE = 512
SUB = 256
GROUPS = ((4, 3), (5, 2), (6, 1), (7, 0))
ARRIVAL = (4, 1, 5, 2, 6, 3, 7)
BF16 = jnp.bfloat16
ANY = pl.BlockSpec(memory_space=pl.ANY)
VMEM = pl.BlockSpec(memory_space=pltpu.VMEM)
SMEM = pl.BlockSpec(memory_space=pltpu.SMEM)


def rate_rows():
    pair = np.arange(128) // 2
    real = pair.astype(np.float64)
    time_rate = np.where(pair < 8, ROPE_THETA ** (-2.0 * real / 16.0), 0.0)
    height_rate = np.where(
        (pair >= 8) & (pair < 36), ROPE_THETA ** (-2.0 * (real - 8.0) / 56.0), 0.0
    )
    width_rate = np.where(pair >= 36, ROPE_THETA ** (-2.0 * (real - 36.0) / 56.0), 0.0)
    return tuple(jnp.asarray(r, jnp.float32) for r in (time_rate, height_rate, width_rate))


def rope_tables(rows, starts, ends, clip_grids):
    inside = ((rows[:, None] >= starts[None, :]) & (rows[:, None] < ends[None, :])).astype(
        jnp.int32
    )
    clip_start = jnp.sum(inside * starts[None, :], axis=1)
    height = jnp.sum(inside * clip_grids[None, :, 0], axis=1)
    breadth = jnp.sum(inside * clip_grids[None, :, 1], axis=1)
    offset = rows - clip_start
    frame = offset // (height * breadth)
    row = offset // breadth % height
    col = offset % breadth
    time_rate, height_rate, width_rate = rate_rows()
    angles = (
        frame.astype(jnp.float32)[:, None] * time_rate[None, :]
        + row.astype(jnp.float32)[:, None] * height_rate[None, :]
        + col.astype(jnp.float32)[:, None] * width_rate[None, :]
    )
    return jnp.cos(angles), jnp.sin(angles)


def rope_body(pos_ref, x_ref, gain_ref, cos_ref, sin_ref, keep_ref, send_ref):
    core = pos_ref[1]
    even = lax.rem(lax.broadcasted_iota(jnp.int32, (SUB, 128), 1), 2) == 0
    for slot, out in ((core, keep_ref), (1 - core, send_ref)):
        x = x_ref[:, pl.ds(pl.multiple_of(slot * 128, 128), 128)].astype(jnp.float32)
        mean = jnp.mean(x * x, axis=-1, keepdims=True)
        x = x * lax.rsqrt(mean + NORM_EPS) * gain_ref[...]
        swapped = jnp.where(even, -pltpu.roll(x, 127, 1), pltpu.roll(x, 1, 1))
        out[0] = (x * cos_ref[...] + swapped * sin_ref[...]).astype(BF16)


def turn_body(pos_ref, x_ref, keep_ref, send_ref):
    core = pos_ref[1]
    for slot, out in ((core, keep_ref), (1 - core, send_ref)):
        out[0] = x_ref[:, pl.ds(pl.multiple_of(slot * 128, 128), 128)].T


def head_blocks(body, pos, x, extra, dims):
    column = lambda k, pos: (0, lax.rem(pos[0] + k, 8))
    fixed = [pl.BlockSpec(e.shape, lambda k, pos: (0, 0)) for e in extra]
    out = jax.ShapeDtypeStruct((8,) + dims, BF16)
    spec = pl.BlockSpec((1,) + dims, lambda k, pos: (k, 0, 0))
    return pl.pallas_call(
        body,
        out_shape=(out, out),
        grid_spec=pltpu.PrefetchScalarGridSpec(
            num_scalar_prefetch=1,
            grid=(8,),
            in_specs=[pl.BlockSpec((SUB, 256), column)] + fixed,
            out_specs=(spec, spec),
        ),
    )(pos, x, *extra)


def attend_body(sc, q0, q1, qse, *refs):
    kv, (o0, o1), scratch = refs[:12], refs[12:14], refs[14:]
    kbuf, vbuf, ksem, vsem, flag, qbuf, acc, s0, s1, p0, p1 = scratch
    zpos, core = sc[0], sc[1]
    scores, probs = (s0, s1), (p0, p1)
    low_all = sc[2] // TILE
    high_all = (sc[5] + TILE - 1) // TILE
    for i in range(1, 4):
        low_all = jnp.minimum(low_all, sc[2 + 4 * i] // TILE)
        high_all = jnp.maximum(high_all, (sc[5 + 4 * i] + TILE - 1) // TILE)

    def start(t, carry):
        pack = t // 8
        rel = lax.rem(t - pack * 8 - zpos + 8, 8)
        half = lax.rem(rel // 2, 2)
        spot = lax.rem(rel, 2) + (rel // 4) * 2
        for n in range(6):

            @pl.when(pack * 2 + half == n)
            def _():
                pltpu.make_async_copy(kv[n].at[spot], kbuf.at[t], ksem.at[t]).start()
                pltpu.make_async_copy(kv[6 + n].at[spot], vbuf.at[t], vsem.at[t]).start()

        flag[t] = 0
        return carry

    lax.fori_loop(low_all, high_all, start, 0)

    def ensure(t):
        @pl.when(flag[t] == 0)
        def _():
            pltpu.make_async_copy(kv[0].at[0], kbuf.at[t], ksem.at[t]).wait()
            pltpu.make_async_copy(kv[6].at[0], vbuf.at[t], vsem.at[t]).wait()
            flag[t] = 1

    qbuf[0:2] = q0[...]
    qbuf[2:4] = q1[...]

    def one(i, carry):
        base = 2 + 4 * i
        low = sc[base] // TILE
        high = (sc[base + 3] + TILE - 1) // TILE
        last_start, first_end = sc[base + 1], sc[base + 2]

        def score(t, into):
            for j in range(2):
                into[pl.ds(SUB * j, SUB), :] = lax.dot_general(
                    kbuf[t, j],
                    qbuf[i],
                    (((1,), (1,)), ((), ())),
                    preferred_element_type=jnp.float32,
                )

        def weigh(t, source):
            return jnp.dot(
                vbuf[t, 0], source[0:SUB, :], preferred_element_type=jnp.float32
            ) + jnp.dot(vbuf[t, 1], source[SUB:TILE, :], preferred_element_type=jnp.float32)

        def step(parity, masked, t, carry):
            top, total, shrink = carry
            score(jnp.minimum(t + 1, high - 1), scores[1 - parity])
            acc[...] = acc[...] * shrink + weigh(jnp.maximum(t - 1, low), probs[1 - parity])
            s = scores[parity][...]
            if masked:
                row = lax.broadcasted_iota(jnp.int32, (TILE, SUB), 0)
                key = (row ^ (core * SUB)) + t * TILE
                s = jnp.where((key >= qse[i, 0:1, :]) & (key < qse[i, 1:2, :]), s, MASK_FLOOR)
            new_top = jnp.maximum(top, jnp.max(s, axis=0, keepdims=True))
            shrink = jnp.exp2((top - new_top) * EXP2_SCALE)
            p = jnp.exp2((s - new_top) * EXP2_SCALE)
            total = total * shrink + jnp.sum(p, axis=0, keepdims=True)
            probs[parity][...] = p.astype(BF16)
            return new_top, total, shrink

        ensure(low)
        score(low, s0)
        acc[...] = jnp.zeros_like(acc)
        p1[...] = jnp.zeros_like(p1)

        def loop(t, carry):
            @pl.when(t + 1 < high)
            def _():
                ensure(t + 1)

            full = (last_start <= t * TILE) & (t * TILE + TILE <= first_end)
            which = lax.rem(t - low, 2) * 2 + jnp.where(full, 0, 1)
            kinds = [
                functools.partial(step, parity, masked, t)
                for parity in (0, 1)
                for masked in (False, True)
            ]
            return lax.switch(which, kinds, carry)

        first = (
            jnp.full((1, SUB), MASK_FLOOR, jnp.float32),
            jnp.zeros((1, SUB), jnp.float32),
            jnp.ones((1, SUB), jnp.float32),
        )
        top, total, shrink = lax.fori_loop(low, high, loop, first)

        def finish(source):
            out = ((acc[...] * shrink + weigh(high - 1, source)) / total).T.astype(BF16)

            @pl.when(i < 2)
            def _():
                o0[jnp.minimum(i, 1)] = out

            @pl.when(i >= 2)
            def _():
                o1[jnp.maximum(i - 2, 0)] = out

        last = lax.rem(high - 1 - low, 2)
        pl.when(last == 0)(lambda: finish(p0))
        pl.when(last == 1)(lambda: finish(p1))
        return carry

    lax.fori_loop(0, 4, one, 0)

    def drain(t, carry):
        ensure(t)
        return carry

    lax.fori_loop(low_all, high_all, drain, 0)


def attend(sc, q0, q1, qse, keys, values):
    block = jax.ShapeDtypeStruct((2, SUB, 128), BF16)
    return pl.pallas_call(
        attend_body,
        out_shape=(block, block),
        in_specs=[SMEM, VMEM, VMEM, VMEM] + [ANY] * 12,
        out_specs=(VMEM, VMEM),
        scratch_shapes=[
            pltpu.VMEM((24, 2, SUB, 128), BF16),
            pltpu.VMEM((24, 2, 128, SUB), BF16),
            pltpu.SemaphoreType.DMA((24,)),
            pltpu.SemaphoreType.DMA((24,)),
            pltpu.SMEM((24,), jnp.int32),
            pltpu.VMEM((4, SUB, 128), BF16),
            pltpu.VMEM((128, SUB), jnp.float32),
            pltpu.VMEM((TILE, SUB), jnp.float32),
            pltpu.VMEM((TILE, SUB), jnp.float32),
            pltpu.VMEM((TILE, SUB), BF16),
            pltpu.VMEM((TILE, SUB), BF16),
        ],
        compiler_params=pltpu.CompilerParams(vmem_limit_bytes=40 << 20),
        cost_estimate=pl.CostEstimate(
            flops=12_000_000_000, transcendentals=4_000_000, bytes_accessed=8_000_000
        ),
    )(sc, q0, q1, qse, *keys, *values)


def place_body(pos_ref, *refs):
    mine, swapped_a, swapped_b, out, sems = refs[:8], refs[8], refs[9], refs[10], refs[11]
    zpos, core = pos_ref[0], pos_ref[1]
    copies = []
    for n, rel in enumerate(RETURN_ORDER):
        head = 2 * lax.rem(zpos + rel, 8)
        other = swapped_a.at[n] if n < 6 else swapped_b.at[n - 6]
        for m, (source, slot) in enumerate(((mine[n].at[0], core), (other, 1 - core))):
            column = pl.multiple_of((head + slot) * 128, 128)
            copy = pltpu.make_async_copy(
                source, out.at[:, pl.ds(column, 128)], sems.at[2 * n + m]
            )
            copy.start()
            copies.append(copy)
    for copy in copies:
        copy.wait()


RETURN_ORDER = tuple((8 - rel) % 8 for group in GROUPS for rel in group)


def place(pos, mine, swapped_a, swapped_b):
    return pl.pallas_call(
        place_body,
        out_shape=jax.ShapeDtypeStruct((SUB, 2048), BF16),
        in_specs=[SMEM] + [ANY] * 10,
        out_specs=ANY,
        scratch_shapes=[pltpu.SemaphoreType.DMA((16,))],
    )(pos, *mine, swapped_a, swapped_b)


def core_swap(x):
    return lax.ppermute(x, "c", [(0, 1), (1, 0)])


def z_shift(x, k):
    return lax.ppermute(x, "z", [(i, (i + k) % 8) for i in range(8)])


def gather_heads(keep, send, order):
    other = core_swap(send)
    arrived = {0: jnp.stack([keep[0], other[0]])}
    for rel in order:
        k = (8 - rel) % 8
        arrived[rel] = z_shift(jnp.stack([keep[k], other[k]]), k)
    return arrived


def with_neighbours(arrived):
    forward = [(i, i + 1) for i in range(15)]
    backward = [(i + 1, i) for i in range(15)]
    halves = [jnp.stack([arrived[r] for r in rels]) for rels in ((0, 1, 4, 5), (2, 3, 6, 7))]
    before = [lax.ppermute(h, "dp", forward) for h in halves]
    after = [lax.ppermute(h, "dp", backward) for h in halves]
    return before + halves + after


def shards(raw_query, raw_key, raw_value, query_gain, key_gain, lengths, clip_grids):
    zpos, core, dpos = lax.axis_index("z"), lax.axis_index("c"), lax.axis_index("dp")
    pos = jnp.stack([zpos, core]).astype(jnp.int32)
    query, key, value = raw_query[0], raw_key[0], raw_value[0]
    ends = jnp.cumsum(lengths).astype(jnp.int32)
    starts = ends - lengths
    pack_base = dpos * 4096
    rows = pack_base + zpos * 512 + core * 256 + jnp.arange(SUB, dtype=jnp.int32)

    value_blocks = head_blocks(turn_body, pos, value, (), (128, SUB))
    cos, sin = rope_tables(rows, starts, ends, clip_grids)
    key_blocks = head_blocks(
        rope_body, pos, key, (key_gain.reshape(1, 128), cos, sin), (SUB, 128)
    )
    query_blocks = head_blocks(
        rope_body, pos, query, (query_gain.reshape(1, 128), cos, sin), (SUB, 128)
    )
    values = gather_heads(*value_blocks, ARRIVAL)
    value_parts = with_neighbours(values)
    keys = gather_heads(*key_blocks, ARRIVAL)
    key_parts = with_neighbours(keys)
    order = [rel for group in GROUPS for rel in group]
    queries = gather_heads(*query_blocks, order[:-1])

    rels = np.array(order, np.int32)
    chip = (zpos + rels) % 8
    side = jnp.stack([core, 1 - core])
    first = pack_base + chip[:, None] * 512 + side[None, :] * 256
    tokens = (first[:, :, None] + jnp.arange(SUB, dtype=jnp.int32)).reshape(16 * SUB)
    base = pack_base - 4096
    began = jnp.max(jnp.where(tokens[:, None] >= starts[None, :], starts[None, :], 0), axis=1)
    ended = jnp.min(jnp.where(tokens[:, None] < ends[None, :], ends[None, :], 65536), axis=1)
    qse = jnp.stack([(began - base).reshape(16, SUB), (ended - base).reshape(16, SUB)], axis=1)
    bounds = qse[:, :, :: SUB - 1].reshape(16, 4)

    returned = []
    for n, (a, b) in enumerate(GROUPS):
        sc = jnp.concatenate([pos, bounds[4 * n : 4 * n + 4].reshape(16)])
        outs = attend(sc, queries[a], queries[b], qse[4 * n : 4 * n + 4], key_parts, value_parts)
        for rel, out in zip((a, b), outs):
            returned.append(z_shift(out, rel) if rel else out)
    swapped_a = core_swap(jnp.stack([r[1] for r in returned[:6]]))
    swapped_b = core_swap(jnp.stack([r[1] for r in returned[6:]]))
    return place(pos, returned, swapped_a, swapped_b).reshape(1, SUB, 2048)


def solution(mesh):
    split = Mesh(mesh.devices.reshape(8, 2, mesh.shape["dp"]), ("z", "c", "dp"))
    token = P("dp", ("z", "c"), None)
    return jax.shard_map(
        shards,
        mesh=split,
        in_specs=(token, token, token, P(), P(), P(), P()),
        out_specs=token,
        check_vma=False,
    )
```

```python
import functools
import math

import jax
import jax.numpy as jnp
import numpy as np
from jax import lax
from jax.experimental import pallas as pl
from jax.experimental.pallas import tpu as pltpu
from jax.sharding import Mesh
from jax.sharding import PartitionSpec as P


NORM_EPS = 1e-06
ROPE_THETA = 256.0
SCORE_SCALE = 1.0 / math.sqrt(128.0)
MASK_FLOOR = -1e30
EXP2_SCALE = SCORE_SCALE * math.log2(math.e)
TILE = 512
SUB = 256
GROUPS = ((0, 2), (4, 3), (5, 6), (7, 1))
ARRIVAL = (1, 7, 2, 6, 3, 5, 4)
PIECES = ((1, 7), (2, 6), (3, 5), (0, 4))
BF16 = jnp.bfloat16
HBM = pl.BlockSpec(memory_space=pltpu.HBM)
VMEM = pl.BlockSpec(memory_space=pltpu.VMEM)
SMEM = pl.BlockSpec(memory_space=pltpu.SMEM)


def rate_rows():
    pair = np.arange(128) // 2
    real = pair.astype(np.float64)
    time_rate = np.where(pair < 8, ROPE_THETA ** (-2.0 * real / 16.0), 0.0)
    height_rate = np.where(
        (pair >= 8) & (pair < 36), ROPE_THETA ** (-2.0 * (real - 8.0) / 56.0), 0.0
    )
    width_rate = np.where(pair >= 36, ROPE_THETA ** (-2.0 * (real - 36.0) / 56.0), 0.0)
    return tuple(jnp.asarray(r, jnp.float32) for r in (time_rate, height_rate, width_rate))


def rope_tables(rows, starts, ends, clip_grids):
    inside = ((rows[:, None] >= starts[None, :]) & (rows[:, None] < ends[None, :])).astype(
        jnp.int32
    )
    clip_start = jnp.sum(inside * starts[None, :], axis=1)
    height = jnp.sum(inside * clip_grids[None, :, 0], axis=1)
    breadth = jnp.sum(inside * clip_grids[None, :, 1], axis=1)
    offset = rows - clip_start
    frame = offset // (height * breadth)
    row = offset // breadth % height
    col = offset % breadth
    time_rate, height_rate, width_rate = rate_rows()
    angles = (
        frame.astype(jnp.float32)[:, None] * time_rate[None, :]
        + row.astype(jnp.float32)[:, None] * height_rate[None, :]
        + col.astype(jnp.float32)[:, None] * width_rate[None, :]
    )
    return jnp.cos(angles), jnp.sin(angles)


def rotate(x, even, gain, cos, sin):
    x = x.astype(jnp.float32)
    mean = jnp.mean(x * x, axis=-1, keepdims=True)
    x = x * lax.rsqrt(mean + NORM_EPS) * gain
    swapped = jnp.where(even, -pltpu.roll(x, 127, 1), pltpu.roll(x, 1, 1))
    return (x * cos + swapped * sin).astype(BF16)


def even_lanes():
    return lax.rem(lax.broadcasted_iota(jnp.int32, (SUB, 128), 1), 2) == 0


def key_value_body(pos, key, value, gain, cos, sin, keep, send):
    even = even_lanes()

    def one(k, carry):
        head = 2 * lax.rem(pos[0] + k, 8)
        for slot, out in ((pos[1], keep), (1 - pos[1], send)):
            column = pl.ds(pl.multiple_of((head + slot) * 128, 128), 128)
            out[k, 0] = rotate(key[:, column], even, gain[...], cos[...], sin[...])
            out[k, 1, 0:128] = value[0:128, column].T
            out[k, 1, 128:256] = value[128:256, column].T
        return carry

    lax.fori_loop(0, 8, one, 0)


def query_body(pos, query, gain, cos, sin, keep, send):
    even = even_lanes()

    def one(k, carry):
        head = 2 * lax.rem(pos[0] + k, 8)
        for slot, out in ((pos[1], keep), (1 - pos[1], send)):
            column = pl.ds(pl.multiple_of((head + slot) * 128, 128), 128)
            out[k] = rotate(query[:, column], even, gain[...], cos[...], sin[...])
        return carry

    lax.fori_loop(0, 8, one, 0)


def head_blocks(body, dims, *args):
    out = jax.ShapeDtypeStruct((8,) + dims, BF16)
    return pl.pallas_call(
        body,
        out_shape=(out, out),
        in_specs=[SMEM] + [VMEM] * (len(args) - 1),
        out_specs=(VMEM, VMEM),
        cost_estimate=pl.CostEstimate(
            flops=2_000_000_000, transcendentals=8192, bytes_accessed=4_000_000
        ),
    )(*args)


def attend_body(sc, q0, q1, qse, *refs):
    kv, (o0, o1), scratch = refs[:12], refs[12:14], refs[14:]
    buf, sem, flag, qbuf, acc, s0, s1, p0, p1 = scratch
    zpos, core = sc[0], sc[1]
    scores, probs = (s0, s1), (p0, p1)
    low_all = sc[2] // TILE
    high_all = (sc[5] + TILE - 1) // TILE
    for i in range(1, 4):
        low_all = jnp.minimum(low_all, sc[2 + 4 * i] // TILE)
        high_all = jnp.maximum(high_all, (sc[5 + 4 * i] + TILE - 1) // TILE)

    def start(t, carry):
        pack = t // 8
        rel = lax.rem(t - pack * 8 - zpos + 8, 8)
        piece = lax.rem(jnp.minimum(rel, 8 - rel) + 3, 4)
        for n in range(12):

            @pl.when(pack * 4 + piece == n)
            def _():
                pltpu.make_async_copy(kv[n].at[rel // 4], buf.at[t], sem.at[t]).start()

        flag[t] = 0
        return carry

    lax.fori_loop(low_all, high_all, start, 0)

    def ensure(t):
        @pl.when(flag[t] == 0)
        def _():
            pltpu.make_async_copy(kv[0].at[0], buf.at[t], sem.at[t]).wait()
            flag[t] = 1

    qbuf[0:2] = q0[...]
    qbuf[2:4] = q1[...]

    def one(i, carry):
        base = 2 + 4 * i
        low = sc[base] // TILE
        high = (sc[base + 3] + TILE - 1) // TILE
        last_start, first_end = sc[base + 1], sc[base + 2]

        def score(t, into):
            for j in range(2):
                into[pl.ds(SUB * j, SUB), :] = lax.dot_general(
                    buf[t, j, 0],
                    qbuf[i],
                    (((1,), (1,)), ((), ())),
                    preferred_element_type=jnp.float32,
                )

        def weigh(t, source):
            parts = []
            for j in range(2):
                turned = jnp.concatenate([buf[t, j, 1, 0:128], buf[t, j, 1, 128:256]], axis=1)
                rows = source[SUB * j : SUB * j + SUB, :]
                parts.append(jnp.dot(turned, rows, preferred_element_type=jnp.float32))
            return parts[0] + parts[1]

        def step(parity, masked, t, carry):
            top, total, shrink = carry
            score(jnp.minimum(t + 1, high - 1), scores[1 - parity])
            acc[...] = acc[...] * shrink + weigh(jnp.maximum(t - 1, low), probs[1 - parity])
            s = scores[parity][...]
            if masked:
                row = lax.broadcasted_iota(jnp.int32, (TILE, SUB), 0)
                key = (row ^ (core * SUB)) + t * TILE
                s = jnp.where((key >= qse[i, 0:1, :]) & (key < qse[i, 1:2, :]), s, MASK_FLOOR)
            new_top = jnp.maximum(top, jnp.max(s, axis=0, keepdims=True))
            shrink = jnp.exp2((top - new_top) * EXP2_SCALE)
            p = jnp.exp2((s - new_top) * EXP2_SCALE)
            total = total * shrink + jnp.sum(p, axis=0, keepdims=True)
            probs[parity][...] = p.astype(BF16)
            return new_top, total, shrink

        ensure(low)
        score(low, s0)
        acc[...] = jnp.zeros_like(acc)
        p1[...] = jnp.zeros_like(p1)

        def loop(t, carry):
            @pl.when(t + 1 < high)
            def _():
                ensure(t + 1)

            full = (last_start <= t * TILE) & (t * TILE + TILE <= first_end)
            which = lax.rem(t - low, 2) * 2 + jnp.where(full, 0, 1)
            kinds = [
                functools.partial(step, parity, masked, t)
                for parity in (0, 1)
                for masked in (False, True)
            ]
            return lax.switch(which, kinds, carry)

        first = (
            jnp.full((1, SUB), MASK_FLOOR, jnp.float32),
            jnp.zeros((1, SUB), jnp.float32),
            jnp.ones((1, SUB), jnp.float32),
        )
        _, total, shrink = lax.fori_loop(low, high, loop, first)

        def finish(source):
            out = ((acc[...] * shrink + weigh(high - 1, source)) / total).T.astype(BF16)

            @pl.when(i < 2)
            def _():
                o0[jnp.minimum(i, 1)] = out

            @pl.when(i >= 2)
            def _():
                o1[jnp.maximum(i - 2, 0)] = out

        last = lax.rem(high - 1 - low, 2)
        pl.when(last == 0)(lambda: finish(p0))
        pl.when(last == 1)(lambda: finish(p1))
        return carry

    lax.fori_loop(0, 4, one, 0)

    def drain(t, carry):
        ensure(t)
        return carry

    lax.fori_loop(low_all, high_all, drain, 0)


def attend(sc, q0, q1, qse, blocks):
    block = jax.ShapeDtypeStruct((2, SUB, 128), BF16)
    return pl.pallas_call(
        attend_body,
        out_shape=(block, block),
        in_specs=[SMEM, VMEM, VMEM, VMEM] + [HBM] * 12,
        out_specs=(VMEM, VMEM),
        scratch_shapes=[
            pltpu.VMEM((24, 2, 2, SUB, 128), BF16),
            pltpu.SemaphoreType.DMA((24,)),
            pltpu.SMEM((24,), jnp.int32),
            pltpu.VMEM((4, SUB, 128), BF16),
            pltpu.VMEM((128, SUB), jnp.float32),
            pltpu.VMEM((TILE, SUB), jnp.float32),
            pltpu.VMEM((TILE, SUB), jnp.float32),
            pltpu.VMEM((TILE, SUB), BF16),
            pltpu.VMEM((TILE, SUB), BF16),
        ],
        compiler_params=pltpu.CompilerParams(vmem_limit_bytes=40 << 20),
        cost_estimate=pl.CostEstimate(
            flops=12_000_000_000, transcendentals=4_000_000, bytes_accessed=8_000_000
        ),
    )(sc, q0, q1, qse, *blocks)


def place_body(pos, *refs):
    mine, swapped_a, swapped_b, out = refs[:8], refs[8], refs[9], refs[10]
    for n, rel in enumerate(RETURN_ORDER):
        head = 2 * lax.rem(pos[0] + rel, 8)
        other = swapped_a[n] if n < 6 else swapped_b[n - 6]
        for block, slot in ((mine[n][0], pos[1]), (other, 1 - pos[1])):
            out[:, pl.ds(pl.multiple_of((head + slot) * 128, 128), 128)] = block


RETURN_ORDER = tuple((8 - rel) % 8 for group in GROUPS for rel in group)


def place(pos, mine, swapped_a, swapped_b):
    return pl.pallas_call(
        place_body,
        out_shape=jax.ShapeDtypeStruct((SUB, 2048), BF16),
        in_specs=[SMEM] + [VMEM] * 10,
        out_specs=VMEM,
    )(pos, *mine, swapped_a, swapped_b)


def core_swap(x):
    return lax.ppermute(x, "c", [(0, 1), (1, 0)])


def z_shift(x, k):
    return lax.ppermute(x, "z", [(i, (i + k) % 8) for i in range(8)])


def gather_heads(keep, send, order):
    other = core_swap(send)
    arrived = {0: jnp.stack([keep[0], other[0]])}
    for rel in order:
        k = (8 - rel) % 8
        block = jnp.stack([keep[k], other[k]])
        arrived[rel] = z_shift(block, k)
    return arrived


def with_neighbours(arrived):
    forward = [(i, i + 1) for i in range(15)]
    backward = [(i + 1, i) for i in range(15)]
    pieces = [jnp.stack([arrived[a], arrived[b]]) for a, b in PIECES]
    before, after = [], []
    for piece in pieces:
        before.append(lax.ppermute(piece, "dp", forward))
        after.append(lax.ppermute(piece, "dp", backward))
    return before + pieces + after


def compute(raw_query, raw_key, raw_value, query_gain, key_gain, lengths, clip_grids):
    zpos, core, dpos = lax.axis_index("z"), lax.axis_index("c"), lax.axis_index("dp")
    pos = jnp.stack([zpos, core]).astype(jnp.int32)
    query, key, value = raw_query[0], raw_key[0], raw_value[0]
    ends = jnp.cumsum(lengths).astype(jnp.int32)
    starts = ends - lengths
    pack_base = dpos * 4096
    rows = pack_base + zpos * 512 + core * 256 + jnp.arange(SUB, dtype=jnp.int32)

    cos, sin = rope_tables(rows, starts, ends, clip_grids)
    blocks = with_neighbours(
        gather_heads(
            *head_blocks(
                key_value_body, (2, SUB, 128), pos, key, value, key_gain.reshape(1, 128), cos, sin
            ),
            ARRIVAL,
        )
    )
    order = [rel for group in GROUPS for rel in group]
    query_blocks = head_blocks(
        query_body, (SUB, 128), pos, query, query_gain.reshape(1, 128), cos, sin
    )
    queries = gather_heads(*query_blocks, order[1:])

    rels = np.array(order, np.int32)
    chip = (zpos + rels) % 8
    side = jnp.stack([core, 1 - core])
    first = pack_base + chip[:, None] * 512 + side[None, :] * 256
    tokens = (first[:, :, None] + jnp.arange(SUB, dtype=jnp.int32)).reshape(16 * SUB)
    base = pack_base - 4096
    began = jnp.max(jnp.where(tokens[:, None] >= starts[None, :], starts[None, :], 0), axis=1)
    ended = jnp.min(jnp.where(tokens[:, None] < ends[None, :], ends[None, :], 65536), axis=1)
    qse = jnp.stack([(began - base).reshape(16, SUB), (ended - base).reshape(16, SUB)], axis=1)
    bounds = qse[:, :, :: SUB - 1].reshape(16, 4)

    returned = []
    for n, (a, b) in enumerate(GROUPS):
        sc = jnp.concatenate([pos, bounds[4 * n : 4 * n + 4].reshape(16)])
        outs = attend(sc, queries[a], queries[b], qse[4 * n : 4 * n + 4], blocks)
        for rel, out in zip((a, b), outs):
            returned.append(z_shift(out, rel) if rel else out)
    swapped_a = core_swap(jnp.stack([r[1] for r in returned[:6]]))
    swapped_b = core_swap(jnp.stack([r[1] for r in returned[6:]]))
    return place(pos, returned, swapped_a, swapped_b).reshape(1, SUB, 2048)


def solution(mesh):
    split = Mesh(mesh.devices.reshape(8, 2, mesh.shape["dp"]), ("z", "c", "dp"))
    token = P("dp", ("z", "c"), None)
    return jax.shard_map(
        compute,
        mesh=split,
        in_specs=(token, token, token, P(), P(), P(), P()),
        out_specs=token,
        check_vma=False,
    )
```

```python
import functools
import math

import jax
import jax.numpy as jnp
import numpy as np
from jax import lax
from jax.experimental import pallas as pl
from jax.experimental.pallas import tpu as pltpu
from jax.sharding import Mesh
from jax.sharding import PartitionSpec as P


NORM_EPS = 1e-06
ROPE_THETA = 256.0
SCORE_SCALE = 1.0 / math.sqrt(128.0)
MASK_FLOOR = -1e30
EXP2_SCALE = SCORE_SCALE * math.log2(math.e)
TILE = 512
SUB = 256
GROUPS = ((0, 2), (4, 3), (5, 6), (7, 1))
ARRIVAL = (1, 7, 2, 6, 3, 5, 4)
PIECES = ((1, 7), (2, 6), (3, 5), (0, 4))
BF16 = jnp.bfloat16
HBM = pl.BlockSpec(memory_space=pltpu.HBM)
VMEM = pl.BlockSpec(memory_space=pltpu.VMEM)
SMEM = pl.BlockSpec(memory_space=pltpu.SMEM)


def rate_rows():
    pair = np.arange(128) // 2
    real = pair.astype(np.float64)
    time_rate = np.where(pair < 8, ROPE_THETA ** (-2.0 * real / 16.0), 0.0)
    height_rate = np.where(
        (pair >= 8) & (pair < 36), ROPE_THETA ** (-2.0 * (real - 8.0) / 56.0), 0.0
    )
    width_rate = np.where(pair >= 36, ROPE_THETA ** (-2.0 * (real - 36.0) / 56.0), 0.0)
    return tuple(jnp.asarray(r, jnp.float32) for r in (time_rate, height_rate, width_rate))


def rope_tables(rows, starts, ends, clip_grids):
    inside = ((rows[:, None] >= starts[None, :]) & (rows[:, None] < ends[None, :])).astype(
        jnp.int32
    )
    clip_start = jnp.sum(inside * starts[None, :], axis=1)
    height = jnp.sum(inside * clip_grids[None, :, 0], axis=1)
    breadth = jnp.sum(inside * clip_grids[None, :, 1], axis=1)
    offset = rows - clip_start
    frame = offset // (height * breadth)
    row = offset // breadth % height
    col = offset % breadth
    time_rate, height_rate, width_rate = rate_rows()
    angles = (
        frame.astype(jnp.float32)[:, None] * time_rate[None, :]
        + row.astype(jnp.float32)[:, None] * height_rate[None, :]
        + col.astype(jnp.float32)[:, None] * width_rate[None, :]
    )
    return jnp.cos(angles), jnp.sin(angles)


def rotate(x, even, gain, cos, sin):
    x = x.astype(jnp.float32)
    mean = jnp.mean(x * x, axis=-1, keepdims=True)
    x = x * lax.rsqrt(mean + NORM_EPS) * gain
    swapped = jnp.where(even, -pltpu.roll(x, 127, 1), pltpu.roll(x, 1, 1))
    return (x * cos + swapped * sin).astype(BF16)


def even_lanes():
    return lax.rem(lax.broadcasted_iota(jnp.int32, (SUB, 128), 1), 2) == 0


def key_value_body(pos, key, value, gain, cos, sin, keep, send):
    even = even_lanes()

    def one(k, carry):
        head = 2 * lax.rem(pos[0] + k, 8)
        for slot, out in ((pos[1], keep), (1 - pos[1], send)):
            column = pl.ds(pl.multiple_of((head + slot) * 128, 128), 128)
            out[k, 0] = rotate(key[:, column], even, gain[...], cos[...], sin[...])
            out[k, 1, 0:128] = value[0:128, column].T
            out[k, 1, 128:256] = value[128:256, column].T
        return carry

    lax.fori_loop(0, 8, one, 0)


def query_body(pos, query, gain, cos, sin, keep, send):
    even = even_lanes()

    def one(k, carry):
        head = 2 * lax.rem(pos[0] + k, 8)
        for slot, out in ((pos[1], keep), (1 - pos[1], send)):
            column = pl.ds(pl.multiple_of((head + slot) * 128, 128), 128)
            out[k] = rotate(query[:, column], even, gain[...], cos[...], sin[...])
        return carry

    lax.fori_loop(0, 8, one, 0)


def head_blocks(body, dims, *args):
    out = jax.ShapeDtypeStruct((8,) + dims, BF16)
    return pl.pallas_call(
        body,
        out_shape=(out, out),
        in_specs=[SMEM] + [VMEM] * (len(args) - 1),
        out_specs=(VMEM, VMEM),
        cost_estimate=pl.CostEstimate(
            flops=2_000_000_000, transcendentals=8192, bytes_accessed=4_000_000
        ),
    )(*args)


def attend_body(sc, q0, q1, qse, *refs):
    kv, (o0, o1), scratch = refs[:12], refs[12:14], refs[14:]
    buf, sem, flag, qbuf, acc, s0, s1, p0, p1 = scratch
    zpos, core = sc[0], sc[1]
    scores, probs = (s0, s1), (p0, p1)
    low_all = sc[2] // TILE
    high_all = (sc[5] + TILE - 1) // TILE
    low_all = jnp.minimum(low_all, sc[6] // TILE)
    high_all = jnp.maximum(high_all, (sc[9] + TILE - 1) // TILE)

    def start(t, carry):
        pack = t // 8
        rel = lax.rem(t - pack * 8 - zpos + 8, 8)
        piece = lax.rem(jnp.minimum(rel, 8 - rel) + 3, 4)
        for n in range(12):

            @pl.when(pack * 4 + piece == n)
            def _():
                pltpu.make_async_copy(kv[n].at[rel // 4], buf.at[t], sem.at[t]).start()

        flag[t] = 0
        return carry

    lax.fori_loop(low_all, high_all, start, 0)

    def ensure(t):
        @pl.when(flag[t] == 0)
        def _():
            pltpu.make_async_copy(kv[0].at[0], buf.at[t], sem.at[t]).wait()
            flag[t] = 1

    qbuf[0] = q0[...].reshape(TILE, 128)
    qbuf[1] = q1[...].reshape(TILE, 128)

    def one(i, carry):
        base = 2 + 4 * i
        low = sc[base] // TILE
        high = (sc[base + 3] + TILE - 1) // TILE
        last_start, first_end = sc[base + 1], sc[base + 2]

        def score(t, into):
            for j in range(2):
                into[pl.ds(SUB * j, SUB), :] = lax.dot_general(
                    buf[t, j, 0],
                    qbuf[i],
                    (((1,), (1,)), ((), ())),
                    preferred_element_type=jnp.float32,
                )

        def weigh(t, source):
            parts = []
            for j in range(2):
                turned = jnp.concatenate([buf[t, j, 1, 0:128], buf[t, j, 1, 128:256]], axis=1)
                rows = source[SUB * j : SUB * j + SUB, :]
                parts.append(jnp.dot(turned, rows, preferred_element_type=jnp.float32))
            return parts[0] + parts[1]

        def step(parity, masked, t, carry):
            top, total, shrink = carry
            score(jnp.minimum(t + 1, high - 1), scores[1 - parity])
            acc[...] = acc[...] * shrink + weigh(jnp.maximum(t - 1, low), probs[1 - parity])
            s = scores[parity][...]
            if masked:
                row = lax.broadcasted_iota(jnp.int32, (TILE, TILE), 0)
                key = (row ^ (core * SUB)) + t * TILE
                s = jnp.where((key >= qse[i, 0:1, :]) & (key < qse[i, 1:2, :]), s, MASK_FLOOR)
            new_top = jnp.maximum(top, jnp.max(s, axis=0, keepdims=True))
            shrink = jnp.exp2((top - new_top) * EXP2_SCALE)
            p = jnp.exp2((s - new_top) * EXP2_SCALE)
            total = total * shrink + jnp.sum(p, axis=0, keepdims=True)
            probs[parity][...] = p.astype(BF16)
            return new_top, total, shrink

        ensure(low)
        score(low, s0)
        acc[...] = jnp.zeros_like(acc)
        p1[...] = jnp.zeros_like(p1)

        def loop(t, carry):
            @pl.when(t + 1 < high)
            def _():
                ensure(t + 1)

            full = (last_start <= t * TILE) & (t * TILE + TILE <= first_end)
            which = lax.rem(t - low, 2) * 2 + jnp.where(full, 0, 1)
            kinds = [
                functools.partial(step, parity, masked, t)
                for parity in (0, 1)
                for masked in (False, True)
            ]
            return lax.switch(which, kinds, carry)

        first = (
            jnp.full((1, TILE), MASK_FLOOR, jnp.float32),
            jnp.zeros((1, TILE), jnp.float32),
            jnp.ones((1, TILE), jnp.float32),
        )
        _, total, shrink = lax.fori_loop(low, high, loop, first)

        @pl.when(lax.rem(high - 1 - low, 2) == 1)
        def _():
            p0[...] = p1[...]

        out = ((acc[...] * shrink + weigh(high - 1, p0)) / total).T.astype(BF16)

        @pl.when(i == 0)
        def _():
            o0[...] = out.reshape(2, SUB, 128)

        @pl.when(i == 1)
        def _():
            o1[...] = out.reshape(2, SUB, 128)

        return carry

    lax.fori_loop(0, 2, one, 0)

    def drain(t, carry):
        ensure(t)
        return carry

    lax.fori_loop(low_all, high_all, drain, 0)


def attend(sc, q0, q1, qse, blocks):
    block = jax.ShapeDtypeStruct((2, SUB, 128), BF16)
    return pl.pallas_call(
        attend_body,
        out_shape=(block, block),
        in_specs=[SMEM, VMEM, VMEM, VMEM] + [HBM] * 12,
        out_specs=(VMEM, VMEM),
        scratch_shapes=[
            pltpu.VMEM((24, 2, 2, SUB, 128), BF16),
            pltpu.SemaphoreType.DMA((24,)),
            pltpu.SMEM((24,), jnp.int32),
            pltpu.VMEM((2, TILE, 128), BF16),
            pltpu.VMEM((128, TILE), jnp.float32),
            pltpu.VMEM((TILE, TILE), jnp.float32),
            pltpu.VMEM((TILE, TILE), jnp.float32),
            pltpu.VMEM((TILE, TILE), BF16),
            pltpu.VMEM((TILE, TILE), BF16),
        ],
        compiler_params=pltpu.CompilerParams(vmem_limit_bytes=40 << 20),
        cost_estimate=pl.CostEstimate(
            flops=12_000_000_000, transcendentals=4_000_000, bytes_accessed=8_000_000
        ),
    )(sc, q0, q1, qse, *blocks)


def place_body(pos, *refs):
    mine, swapped_a, swapped_b, out = refs[:8], refs[8], refs[9], refs[10]
    for n, rel in enumerate(RETURN_ORDER):
        head = 2 * lax.rem(pos[0] + rel, 8)
        other = swapped_a[n] if n < 6 else swapped_b[n - 6]
        for block, slot in ((mine[n][0], pos[1]), (other, 1 - pos[1])):
            out[:, pl.ds(pl.multiple_of((head + slot) * 128, 128), 128)] = block


RETURN_ORDER = tuple((8 - rel) % 8 for group in GROUPS for rel in group)


def place(pos, mine, swapped_a, swapped_b):
    return pl.pallas_call(
        place_body,
        out_shape=jax.ShapeDtypeStruct((SUB, 2048), BF16),
        in_specs=[SMEM] + [VMEM] * 10,
        out_specs=VMEM,
    )(pos, *mine, swapped_a, swapped_b)


def core_swap(x):
    return lax.ppermute(x, "c", [(0, 1), (1, 0)])


def z_shift(x, k):
    return lax.ppermute(x, "z", [(i, (i + k) % 8) for i in range(8)])


def gather_heads(keep, send, order):
    other = core_swap(send)
    arrived = {0: jnp.stack([keep[0], other[0]])}
    for rel in order:
        k = (8 - rel) % 8
        block = jnp.stack([keep[k], other[k]])
        arrived[rel] = z_shift(block, k)
    return arrived


def with_neighbours(arrived):
    forward = [(i, i + 1) for i in range(15)]
    backward = [(i + 1, i) for i in range(15)]
    pieces = [jnp.stack([arrived[a], arrived[b]]) for a, b in PIECES]
    before, after = [], []
    for piece in pieces:
        before.append(lax.ppermute(piece, "dp", forward))
        after.append(lax.ppermute(piece, "dp", backward))
    return before + pieces + after


def compute(raw_query, raw_key, raw_value, query_gain, key_gain, lengths, clip_grids):
    zpos, core, dpos = lax.axis_index("z"), lax.axis_index("c"), lax.axis_index("dp")
    pos = jnp.stack([zpos, core]).astype(jnp.int32)
    query, key, value = raw_query[0], raw_key[0], raw_value[0]
    ends = jnp.cumsum(lengths).astype(jnp.int32)
    starts = ends - lengths
    pack_base = dpos * 4096
    rows = pack_base + zpos * 512 + core * 256 + jnp.arange(SUB, dtype=jnp.int32)

    cos, sin = rope_tables(rows, starts, ends, clip_grids)
    blocks = with_neighbours(
        gather_heads(
            *head_blocks(
                key_value_body, (2, SUB, 128), pos, key, value, key_gain.reshape(1, 128), cos, sin
            ),
            ARRIVAL,
        )
    )
    order = [rel for group in GROUPS for rel in group]
    query_blocks = head_blocks(
        query_body, (SUB, 128), pos, query, query_gain.reshape(1, 128), cos, sin
    )
    queries = gather_heads(*query_blocks, order[1:])

    rels = np.array(order, np.int32)
    chip = (zpos + rels) % 8
    side = jnp.stack([core, 1 - core])
    first = pack_base + chip[:, None] * 512 + side[None, :] * 256
    tokens = (first[:, :, None] + jnp.arange(SUB, dtype=jnp.int32)).reshape(16 * SUB)
    base = pack_base - 4096
    began = jnp.max(jnp.where(tokens[:, None] >= starts[None, :], starts[None, :], 0), axis=1)
    ended = jnp.min(jnp.where(tokens[:, None] < ends[None, :], ends[None, :], 65536), axis=1)
    began = (began - base).reshape(8, TILE)
    ended = (ended - base).reshape(8, TILE)
    qse = jnp.stack([began, ended], axis=1)
    bounds = jnp.stack(
        [began.min(axis=1), began.max(axis=1), ended.min(axis=1), ended.max(axis=1)], axis=1
    )

    returned = []
    for n, (a, b) in enumerate(GROUPS):
        sc = jnp.concatenate([pos, bounds[2 * n : 2 * n + 2].reshape(8)])
        outs = attend(sc, queries[a], queries[b], qse[2 * n : 2 * n + 2], blocks)
        for rel, out in zip((a, b), outs):
            returned.append(z_shift(out, rel) if rel else out)
    swapped_a = core_swap(jnp.stack([r[1] for r in returned[:6]]))
    swapped_b = core_swap(jnp.stack([r[1] for r in returned[6:]]))
    return place(pos, returned, swapped_a, swapped_b).reshape(1, SUB, 2048)


def solution(mesh):
    split = Mesh(mesh.devices.reshape(8, 2, mesh.shape["dp"]), ("z", "c", "dp"))
    token = P("dp", ("z", "c"), None)
    return jax.shard_map(
        compute,
        mesh=split,
        in_specs=(token, token, token, P(), P(), P(), P()),
        out_specs=token,
        check_vma=False,
    )
```

```python
import functools
import math

import jax
import jax.numpy as jnp
import numpy as np
from jax import lax
from jax.experimental import pallas as pl
from jax.experimental.pallas import tpu as pltpu
from jax.sharding import Mesh
from jax.sharding import PartitionSpec as P


NORM_EPS = 1e-06
ROPE_THETA = 256.0
SCORE_SCALE = 1.0 / math.sqrt(128.0)
MASK_FLOOR = -1e30
EXP2_SCALE = SCORE_SCALE * math.log2(math.e)
TILE = 512
SUB = 256
GROUPS = ((0, 2), (4, 3), (5, 6), (7, 1))
ARRIVAL = (1, 7, 2, 6, 3, 5, 4)
PIECES = ((1, 2, 6, 7), (0, 3, 4, 5))
BF16 = jnp.bfloat16
HBM = pl.BlockSpec(memory_space=pltpu.HBM)
VMEM = pl.BlockSpec(memory_space=pltpu.VMEM)
SMEM = pl.BlockSpec(memory_space=pltpu.SMEM)


def rate_rows():
    pair = np.arange(128) // 2
    real = pair.astype(np.float64)
    time_rate = np.where(pair < 8, ROPE_THETA ** (-2.0 * real / 16.0), 0.0)
    height_rate = np.where(
        (pair >= 8) & (pair < 36), ROPE_THETA ** (-2.0 * (real - 8.0) / 56.0), 0.0
    )
    width_rate = np.where(pair >= 36, ROPE_THETA ** (-2.0 * (real - 36.0) / 56.0), 0.0)
    return tuple(jnp.asarray(r, jnp.float32) for r in (time_rate, height_rate, width_rate))


def rope_tables(rows, starts, ends, clip_grids):
    inside = ((rows[:, None] >= starts[None, :]) & (rows[:, None] < ends[None, :])).astype(
        jnp.int32
    )
    clip_start = jnp.sum(inside * starts[None, :], axis=1)
    height = jnp.sum(inside * clip_grids[None, :, 0], axis=1)
    breadth = jnp.sum(inside * clip_grids[None, :, 1], axis=1)
    offset = rows - clip_start
    frame = offset // (height * breadth)
    row = offset // breadth % height
    col = offset % breadth
    time_rate, height_rate, width_rate = rate_rows()
    angles = (
        frame.astype(jnp.float32)[:, None] * time_rate[None, :]
        + row.astype(jnp.float32)[:, None] * height_rate[None, :]
        + col.astype(jnp.float32)[:, None] * width_rate[None, :]
    )
    return jnp.cos(angles), jnp.sin(angles)


def rotate(x, even, gain, cos, sin):
    x = x.astype(jnp.float32)
    mean = jnp.mean(x * x, axis=-1, keepdims=True)
    x = x * lax.rsqrt(mean + NORM_EPS) * gain
    swapped = jnp.where(even, -pltpu.roll(x, 127, 1), pltpu.roll(x, 1, 1))
    return (x * cos + swapped * sin).astype(BF16)


def even_lanes():
    return lax.rem(lax.broadcasted_iota(jnp.int32, (SUB, 128), 1), 2) == 0


def key_value_body(pos, key, value, gain, cos, sin, keep, send):
    even = even_lanes()

    def one(k, carry):
        head = 2 * lax.rem(pos[0] + k, 8)
        for slot, out in ((pos[1], keep), (1 - pos[1], send)):
            column = pl.ds(pl.multiple_of((head + slot) * 128, 128), 128)
            out[k, 0] = rotate(key[:, column], even, gain[...], cos[...], sin[...])
            out[k, 1, 0:128] = value[0:128, column].T
            out[k, 1, 128:256] = value[128:256, column].T
        return carry

    lax.fori_loop(0, 8, one, 0)


def query_body(pos, query, gain, cos, sin, keep, send):
    even = even_lanes()

    def one(k, carry):
        head = 2 * lax.rem(pos[0] + k, 8)
        for slot, out in ((pos[1], keep), (1 - pos[1], send)):
            column = pl.ds(pl.multiple_of((head + slot) * 128, 128), 128)
            out[k] = rotate(query[:, column], even, gain[...], cos[...], sin[...])
        return carry

    lax.fori_loop(0, 8, one, 0)


def head_blocks(body, dims, *args):
    out = jax.ShapeDtypeStruct((8,) + dims, BF16)
    return pl.pallas_call(
        body,
        out_shape=(out, out),
        in_specs=[SMEM] + [VMEM] * (len(args) - 1),
        out_specs=(VMEM, VMEM),
        cost_estimate=pl.CostEstimate(
            flops=2_000_000_000, transcendentals=8192, bytes_accessed=4_000_000
        ),
    )(*args)


def attend_body(sc, q0, q1, qse, *refs):
    kv, (o0, o1), scratch = refs[:6], refs[6:8], refs[8:]
    buf, sem, flag, qbuf, acc, s0, s1, p0, p1 = scratch
    zpos, core = sc[0], sc[1]
    scores, probs = (s0, s1), (p0, p1)
    low_all = sc[2] // TILE
    high_all = (sc[5] + TILE - 1) // TILE
    low_all = jnp.minimum(low_all, sc[6] // TILE)
    high_all = jnp.maximum(high_all, (sc[9] + TILE - 1) // TILE)

    def start(t, carry):
        pack = t // 8
        rel = lax.rem(t - pack * 8 - zpos + 8, 8)
        away = jnp.minimum(rel, 8 - rel)
        near = jnp.where((away == 1) | (away == 2), 0, 1)
        spot = jnp.where(near == 0, jnp.where(rel < 4, rel - 1, rel - 4), jnp.where(rel == 0, 0, rel - 2))
        for n in range(6):

            @pl.when(pack * 2 + near == n)
            def _():
                pltpu.make_async_copy(kv[n].at[spot], buf.at[t], sem.at[t]).start()

        flag[t] = 0
        return carry

    lax.fori_loop(low_all, high_all, start, 0)

    def ensure(t):
        @pl.when(flag[t] == 0)
        def _():
            pltpu.make_async_copy(kv[0].at[0], buf.at[t], sem.at[t]).wait()
            flag[t] = 1

    qbuf[0] = q0[...].reshape(TILE, 128)
    qbuf[1] = q1[...].reshape(TILE, 128)

    def one(i, carry):
        base = 2 + 4 * i
        low = sc[base] // TILE
        high = (sc[base + 3] + TILE - 1) // TILE
        last_start, first_end = sc[base + 1], sc[base + 2]

        def score(t, into):
            for j in range(2):
                into[pl.ds(SUB * j, SUB), :] = lax.dot_general(
                    buf[t, j, 0],
                    qbuf[i],
                    (((1,), (1,)), ((), ())),
                    preferred_element_type=jnp.float32,
                )

        def weigh(t, source):
            parts = []
            for j in range(2):
                turned = jnp.concatenate([buf[t, j, 1, 0:128], buf[t, j, 1, 128:256]], axis=1)
                rows = source[SUB * j : SUB * j + SUB, :]
                parts.append(jnp.dot(turned, rows, preferred_element_type=jnp.float32))
            return parts[0] + parts[1]

        def step(parity, masked, t, carry):
            top, total, shrink = carry
            score(jnp.minimum(t + 1, high - 1), scores[1 - parity])
            acc[...] = acc[...] * shrink + weigh(jnp.maximum(t - 1, low), probs[1 - parity])
            s = scores[parity][...]
            if masked:
                row = lax.broadcasted_iota(jnp.int32, (TILE, TILE), 0)
                key = (row ^ (core * SUB)) + t * TILE
                s = jnp.where((key >= qse[i, 0:1, :]) & (key < qse[i, 1:2, :]), s, MASK_FLOOR)
            new_top = jnp.maximum(top, jnp.max(s, axis=0, keepdims=True))
            shrink = jnp.exp2((top - new_top) * EXP2_SCALE)
            p = jnp.exp2((s - new_top) * EXP2_SCALE)
            total = total * shrink + jnp.sum(p, axis=0, keepdims=True)
            probs[parity][...] = p.astype(BF16)
            return new_top, total, shrink

        ensure(low)
        score(low, s0)
        acc[...] = jnp.zeros_like(acc)
        p1[...] = jnp.zeros_like(p1)

        def loop(t, carry):
            @pl.when(t + 1 < high)
            def _():
                ensure(t + 1)

            full = (last_start <= t * TILE) & (t * TILE + TILE <= first_end)
            which = lax.rem(t - low, 2) * 2 + jnp.where(full, 0, 1)
            kinds = [
                functools.partial(step, parity, masked, t)
                for parity in (0, 1)
                for masked in (False, True)
            ]
            return lax.switch(which, kinds, carry)

        first = (
            jnp.full((1, TILE), MASK_FLOOR, jnp.float32),
            jnp.zeros((1, TILE), jnp.float32),
            jnp.ones((1, TILE), jnp.float32),
        )
        _, total, shrink = lax.fori_loop(low, high, loop, first)

        @pl.when(lax.rem(high - 1 - low, 2) == 1)
        def _():
            p0[...] = p1[...]

        out = ((acc[...] * shrink + weigh(high - 1, p0)) / total).T.astype(BF16)

        @pl.when(i == 0)
        def _():
            o0[...] = out.reshape(2, SUB, 128)

        @pl.when(i == 1)
        def _():
            o1[...] = out.reshape(2, SUB, 128)

        return carry

    lax.fori_loop(0, 2, one, 0)

    def drain(t, carry):
        ensure(t)
        return carry

    lax.fori_loop(low_all, high_all, drain, 0)


def attend(sc, q0, q1, qse, blocks):
    block = jax.ShapeDtypeStruct((2, SUB, 128), BF16)
    return pl.pallas_call(
        attend_body,
        out_shape=(block, block),
        in_specs=[SMEM, VMEM, VMEM, VMEM] + [HBM] * 6,
        out_specs=(VMEM, VMEM),
        scratch_shapes=[
            pltpu.VMEM((24, 2, 2, SUB, 128), BF16),
            pltpu.SemaphoreType.DMA((24,)),
            pltpu.SMEM((24,), jnp.int32),
            pltpu.VMEM((2, TILE, 128), BF16),
            pltpu.VMEM((128, TILE), jnp.float32),
            pltpu.VMEM((TILE, TILE), jnp.float32),
            pltpu.VMEM((TILE, TILE), jnp.float32),
            pltpu.VMEM((TILE, TILE), BF16),
            pltpu.VMEM((TILE, TILE), BF16),
        ],
        compiler_params=pltpu.CompilerParams(vmem_limit_bytes=40 << 20),
        cost_estimate=pl.CostEstimate(
            flops=12_000_000_000, transcendentals=4_000_000, bytes_accessed=8_000_000
        ),
    )(sc, q0, q1, qse, *blocks)


def place_body(pos, *refs):
    mine, swapped_a, swapped_b, out = refs[:8], refs[8], refs[9], refs[10]
    for n, rel in enumerate(RETURN_ORDER):
        head = 2 * lax.rem(pos[0] + rel, 8)
        other = swapped_a[n] if n < 6 else swapped_b[n - 6]
        for block, slot in ((mine[n][0], pos[1]), (other, 1 - pos[1])):
            out[:, pl.ds(pl.multiple_of((head + slot) * 128, 128), 128)] = block


RETURN_ORDER = tuple((8 - rel) % 8 for group in GROUPS for rel in group)


def place(pos, mine, swapped_a, swapped_b):
    return pl.pallas_call(
        place_body,
        out_shape=jax.ShapeDtypeStruct((SUB, 2048), BF16),
        in_specs=[SMEM] + [VMEM] * 10,
        out_specs=VMEM,
    )(pos, *mine, swapped_a, swapped_b)


def core_swap(x):
    return lax.ppermute(x, "c", [(0, 1), (1, 0)])


def z_shift(x, k):
    return lax.ppermute(x, "z", [(i, (i + k) % 8) for i in range(8)])


def gather_heads(keep, send, order):
    other = core_swap(send)
    arrived = {0: jnp.stack([keep[0], other[0]])}
    for rel in order:
        k = (8 - rel) % 8
        block = jnp.stack([keep[k], other[k]])
        arrived[rel] = z_shift(block, k)
    return arrived


def with_neighbours(arrived):
    forward = [(i, i + 1) for i in range(15)]
    backward = [(i + 1, i) for i in range(15)]
    pieces = [jnp.stack([arrived[r] for r in rels]) for rels in PIECES]
    before, after = [], []
    for piece in pieces:
        before.append(lax.ppermute(piece, "dp", forward))
        after.append(lax.ppermute(piece, "dp", backward))
    return before + pieces + after


def compute(raw_query, raw_key, raw_value, query_gain, key_gain, lengths, clip_grids):
    zpos, core, dpos = lax.axis_index("z"), lax.axis_index("c"), lax.axis_index("dp")
    pos = jnp.stack([zpos, core]).astype(jnp.int32)
    query, key, value = raw_query[0], raw_key[0], raw_value[0]
    ends = jnp.cumsum(lengths).astype(jnp.int32)
    starts = ends - lengths
    pack_base = dpos * 4096
    rows = pack_base + zpos * 512 + core * 256 + jnp.arange(SUB, dtype=jnp.int32)

    cos, sin = rope_tables(rows, starts, ends, clip_grids)
    blocks = with_neighbours(
        gather_heads(
            *head_blocks(
                key_value_body, (2, SUB, 128), pos, key, value, key_gain.reshape(1, 128), cos, sin
            ),
            ARRIVAL,
        )
    )
    order = [rel for group in GROUPS for rel in group]
    query_blocks = head_blocks(
        query_body, (SUB, 128), pos, query, query_gain.reshape(1, 128), cos, sin
    )
    queries = gather_heads(*query_blocks, order[1:])

    rels = np.array(order, np.int32)
    chip = (zpos + rels) % 8
    side = jnp.stack([core, 1 - core])
    first = pack_base + chip[:, None] * 512 + side[None, :] * 256
    tokens = (first[:, :, None] + jnp.arange(SUB, dtype=jnp.int32)).reshape(16 * SUB)
    base = pack_base - 4096
    began = jnp.max(jnp.where(tokens[:, None] >= starts[None, :], starts[None, :], 0), axis=1)
    ended = jnp.min(jnp.where(tokens[:, None] < ends[None, :], ends[None, :], 65536), axis=1)
    began = (began - base).reshape(8, TILE)
    ended = (ended - base).reshape(8, TILE)
    qse = jnp.stack([began, ended], axis=1)
    bounds = jnp.stack(
        [began.min(axis=1), began.max(axis=1), ended.min(axis=1), ended.max(axis=1)], axis=1
    )

    returned = []
    for n, (a, b) in enumerate(GROUPS):
        sc = jnp.concatenate([pos, bounds[2 * n : 2 * n + 2].reshape(8)])
        outs = attend(sc, queries[a], queries[b], qse[2 * n : 2 * n + 2], blocks)
        for rel, out in zip((a, b), outs):
            returned.append(z_shift(out, rel) if rel else out)
    swapped_a = core_swap(jnp.stack([r[1] for r in returned[:6]]))
    swapped_b = core_swap(jnp.stack([r[1] for r in returned[6:]]))
    return place(pos, returned, swapped_a, swapped_b).reshape(1, SUB, 2048)


def solution(mesh):
    split = Mesh(mesh.devices.reshape(8, 2, mesh.shape["dp"]), ("z", "c", "dp"))
    token = P("dp", ("z", "c"), None)
    return jax.shard_map(
        compute,
        mesh=split,
        in_specs=(token, token, token, P(), P(), P(), P()),
        out_specs=token,
        check_vma=False,
    )
```
